128 devices in a mesh: slab: 4 (over x_hi, core), img: 32 (over z, y, x_lo).
Axes of the slice: x: 4 (x_hi: 2, x_lo: 2; x = x_hi * 2 + x_lo), y: 4, z: 4, core: 2. Of those that a mesh axis runs over, the one named last changes fastest.
Arguments:
- feats: bfloat16 [32, 32, 128, 512], P('img', 'slab'), may hold values from -6 to 6
- labels: int32 [32], P('img'), may hold values from 0 to 999
- conv_w: bfloat16 [9, 512, 4], replicated, may hold values from -0.09375 to 0.09375
- embed_w: bfloat16 [16, 1024], replicated, may hold values from -1.5 to 1.5
- mod_table: bfloat16 [1000, 2048], replicated, may hold values from -3 to 3
- qkv_w: bfloat16 [1024, 3072], replicated, may hold values from -0.1875 to 0.1875
- out_w: bfloat16 [1024, 1024], replicated, may hold values from -0.1875 to 0.1875
- proj_w: bfloat16 [1024, 768], replicated, may hold values from -0.1875 to 0.1875
- dino: bfloat16 [32, 1024, 768], P('img', 'slab'), may hold values from -6 to 6
Outputs:
- grad_feats: bfloat16 [32, 32, 128, 512], P('img', 'slab')
- grad_proj: float32 [1024, 768], replicated
- grad_conv: float32 [9, 512, 4], replicated
- loss: float32 [], replicated
The draws below stay inside these ranges and needn't reach their ends.
All inputs are finite; a program needn't handle non-finite values.
Results may differ from the reference program's by a relative error of at most 0.024.
Values may be sent and summed in bfloat16 or wider, within the bound.
No kernel may reach another device: no remote copies, remote signals or barrier semaphores. Data moves between devices by JAX's collectives and lax.ppermute only.
A program may use at most 128 MiB of HBM per device.

```python
import jax
import jax.numpy as jnp
from jax import lax

C = 512
LAT = 4
D = 1024
HEAD_DIM = 64
DINO = 768
CLASSES = 1000
WL = 128
HL = 32
TOK_IMG = 1024
IMAGES = 32


def place_ends(drawn, own_key, low, high):
    extent = drawn.shape
    spot = [jax.random.randint(jax.random.fold_in(own_key, axis), (), 0, extent[axis]) for axis in range(len(extent))]
    drawn = drawn.at[tuple(spot)].set(low)
    longest = extent.index(max(extent))
    spot[longest] = (spot[longest] + 1) % extent[longest]
    return drawn.at[tuple(spot)].set(high)


def levels(own_key, shape, split, smallest, high):
    def one(position, blocks):
        draws = jax.random.uniform(jax.random.fold_in(jax.random.fold_in(own_key, 6), position), (blocks,), jnp.float32, smallest / len(split), high / len(split))
        return jnp.repeat(jnp.exp(draws), shape[position] // blocks).reshape((-1,) + (1,) * (len(shape) - position - 1))

    factor_of = one(*split[0])
    for cut in split[1:]:
        factor_of = factor_of * one(*cut)
    return factor_of


def centred(key, extent, scale, reach, shards=(), kind=jnp.bfloat16):
    values = scale * jax.random.normal(key, extent, jnp.float32)
    if shards:
        values = values * levels(key, extent, shards, -0.22, 0.18)
    return jnp.clip(values, -reach, reach).astype(kind)


def setup_inputs(seed: int = 0) -> dict:
    keys = jax.random.split(jax.random.key(seed), 10)
    return {
        "feats": centred(keys[0], (IMAGES, HL, WL, C), 1.0, 6.0, ((0, 32), (1, 4))),
        "labels": place_ends(jax.random.randint(keys[1], (IMAGES,), 0, CLASSES), jax.random.fold_in(keys[1], 1), 0, CLASSES - 1).astype(jnp.int32),
        "conv_w": centred(keys[2], (9, C, LAT), (9 * C) ** -0.5, 0.09375),
        "embed_w": centred(keys[3], (4 * LAT, D), (4 * LAT) ** -0.5, 1.5),
        "mod_table": centred(keys[4], (CLASSES, 2 * D), 0.5, 3.0),
        "qkv_w": centred(keys[5], (D, 3 * D), D ** -0.5, 0.1875),
        "out_w": centred(keys[6], (D, D), D ** -0.5, 0.1875),
        "proj_w": centred(keys[7], (D, DINO), D ** -0.5, 0.1875),
        "dino": centred(keys[8], (IMAGES, TOK_IMG, DINO), 1.0, 6.0, ((0, 32), (1, 4))),
    }


latent_scale = 0.18215
norm_eps = 1e-06
cosine_eps = 1e-06

def conv_out(padded, conv_w):
    rows = padded.shape[0] - 2
    cols = padded.shape[1] - 2
    total = jnp.zeros((rows * cols, conv_w.shape[2]), jnp.float32)
    for tap in range(9):
        view = padded[tap // 3:tap // 3 + rows, tap % 3:tap % 3 + cols]
        total = total + jnp.dot(view.reshape(rows * cols, -1), conv_w[tap], preferred_element_type=jnp.float32)
    return total.reshape(rows, cols, -1) * latent_scale

def conv_back(padded, grad_pad, conv_w):
    rows = grad_pad.shape[0] - 2
    cols = grad_pad.shape[1] - 2
    center = grad_pad[1:-1, 1:-1].reshape(rows * cols, -1)
    grad_in = jnp.zeros((rows * cols, conv_w.shape[1]), jnp.float32)
    parts = []
    for tap in range(9):
        row_off = tap // 3
        col_off = tap % 3
        g_view = grad_pad[2 - row_off:2 - row_off + rows, 2 - col_off:2 - col_off + cols].reshape(rows * cols, -1)
        grad_in = grad_in + jnp.dot(g_view, conv_w[tap].T, preferred_element_type=jnp.float32)
        f_view = padded[row_off:row_off + rows, col_off:col_off + cols].reshape(rows * cols, -1)
        parts.append(jnp.dot(f_view.T, center, preferred_element_type=jnp.float32))
    return (grad_in.reshape(rows, cols, -1), jnp.stack(parts, 0))

def patchify(latent):
    rows, cols, chans = latent.shape
    blocks = latent.reshape(rows // 2, 2, cols // 2, 2, chans).transpose(0, 2, 1, 3, 4)
    return blocks.reshape(rows // 2 * (cols // 2), 4 * chans)

def unpatchify(tokens, rows, cols):
    chans = tokens.shape[1] // 4
    blocks = tokens.reshape(rows // 2, cols // 2, 2, 2, chans).transpose(0, 2, 1, 3, 4)
    return blocks.reshape(rows, cols, chans)

def cosine_grad(projected, target):
    norm_p = jnp.sqrt(lax.optimization_barrier(jnp.sum(projected * projected, -1, keepdims=True)) + cosine_eps)
    norm_t = jnp.sqrt(lax.optimization_barrier(jnp.sum(target * target, -1, keepdims=True)) + cosine_eps)
    cosine = lax.optimization_barrier(jnp.sum(projected * target, -1, keepdims=True)) / (norm_p * norm_t)
    grad = cosine * projected / (norm_p * norm_p) - target / (norm_p * norm_t)
    return (cosine[:, 0], grad)

def widen(x):
    return lax.optimization_barrier(x.astype(jnp.bfloat16)).astype(jnp.float32)

def one_image(image, label, target_b, conv_w, embed_w, mod_table, qkv_w, out_w, proj_w):
    rows, cols, chans = image.shape
    width = qkv_w.shape[0]
    heads = width // HEAD_DIM
    scale = HEAD_DIM ** (-0.5)
    padded = jnp.pad(image, ((1, 1), (1, 1), (0, 0)))
    tokens = patchify(conv_out(padded, conv_w))
    count = tokens.shape[0]
    embed_f = embed_w.astype(jnp.float32)
    start = jnp.dot(tokens, embed_f, precision=lax.Precision.HIGHEST)
    row = mod_table[label].astype(jnp.float32)
    mean = lax.optimization_barrier(jnp.mean(start, -1, keepdims=True))
    cent = start - mean
    inv = lax.rsqrt(lax.optimization_barrier(jnp.mean(cent * cent, -1, keepdims=True)) + norm_eps)
    normed = cent * inv
    modded = (normed * (1.0 + row[width:]) + row[:width]).astype(jnp.bfloat16)
    qkv = jnp.dot(modded, qkv_w, preferred_element_type=jnp.float32).astype(jnp.bfloat16)
    q3 = qkv[:, :width].astype(jnp.float32).reshape(count, heads, HEAD_DIM)
    k3 = qkv[:, width:2 * width].astype(jnp.float32).reshape(count, heads, HEAD_DIM)
    v3 = qkv[:, 2 * width:].astype(jnp.float32).reshape(count, heads, HEAD_DIM)
    scores = jnp.einsum('qhd,khd->hqk', q3, k3) * scale
    top = lax.optimization_barrier(jnp.max(scores, -1, keepdims=True))
    expo = jnp.exp(scores - top)
    total = lax.optimization_barrier(jnp.sum(expo, -1))
    attended = jnp.einsum('hqk,khd->qhd', widen(expo), v3) / total.T[:, :, None]
    attended = attended.reshape(count, width).astype(jnp.bfloat16)
    lse = top[..., 0] + jnp.log(total)
    resid = start + jnp.dot(attended, out_w, preferred_element_type=jnp.float32)
    resid_b = resid.astype(jnp.bfloat16)
    projected = jnp.dot(resid_b, proj_w, preferred_element_type=jnp.float32)
    cosine, grad_p = cosine_grad(projected, target_b.astype(jnp.float32))
    grad_pb = grad_p.astype(jnp.bfloat16)
    proj_part = jnp.dot(resid_b.T, grad_pb, preferred_element_type=jnp.float32)
    grad_resid = jnp.dot(grad_pb, proj_w.T, preferred_element_type=jnp.float32)
    grad_att = jnp.dot(grad_resid.astype(jnp.bfloat16), out_w.T, preferred_element_type=jnp.float32).astype(jnp.bfloat16)
    g3 = grad_att.astype(jnp.float32).reshape(count, heads, HEAD_DIM)
    delta = lax.optimization_barrier(jnp.sum(g3 * attended.astype(jnp.float32).reshape(count, heads, HEAD_DIM), -1)).T
    probs = jnp.exp(scores - lse[..., None])
    dprobs = jnp.einsum('qhd,khd->hqk', g3, v3)
    dscores = widen(probs * (dprobs - delta[..., None]))
    grad_q = scale * jnp.einsum('hqk,khd->qhd', dscores, k3).reshape(count, width)
    grad_k = scale * jnp.einsum('hqk,qhd->khd', dscores, q3).reshape(count, width)
    grad_v = jnp.einsum('hqk,qhd->khd', widen(probs), g3).reshape(count, width)
    grad_qkv = jnp.concatenate([grad_q, grad_k, grad_v], 1).astype(jnp.bfloat16)
    grad_mod = jnp.dot(grad_qkv, qkv_w.T, preferred_element_type=jnp.float32)
    grad_norm = grad_mod * (1.0 + row[width:])
    grad_start = grad_resid + inv * (grad_norm - lax.optimization_barrier(jnp.mean(grad_norm, -1, keepdims=True)) - normed * lax.optimization_barrier(jnp.mean(grad_norm * normed, -1, keepdims=True)))
    grad_tokens = jnp.dot(grad_start, embed_f.T, precision=lax.Precision.HIGHEST)
    grad_latent = (unpatchify(grad_tokens, rows, cols) * latent_scale).astype(jnp.bfloat16)
    grad_pad = jnp.pad(grad_latent, ((1, 1), (1, 1), (0, 0)))
    grad_image, conv_part = conv_back(padded, grad_pad, conv_w)
    return (grad_image.astype(jnp.bfloat16), proj_part, conv_part, jnp.sum(1.0 - cosine))

def reference(feats, labels, conv_w, embed_w, mod_table, qkv_w, out_w, proj_w, dino):

    def step(args):
        image, label, target = args
        return one_image(image, label, target, conv_w, embed_w, mod_table, qkv_w, out_w, proj_w)
    grads, proj_parts, conv_parts, losses = lax.map(step, (feats, labels, dino))
    loss = jnp.sum(losses) / (IMAGES * TOK_IMG)
    return (grads, lax.optimization_barrier(jnp.sum(proj_parts, 0)), lax.optimization_barrier(jnp.sum(conv_parts, 0)), loss)
```

```python
import functools
import jax
import jax.numpy as jnp
from jax import lax
from jax.experimental import pallas as pl
from jax.experimental.pallas import tpu as pltpu
from jax.sharding import Mesh
from jax.sharding import PartitionSpec as P

HEAD_DIM = 64
latent_scale = 0.18215
norm_eps = 1e-06
cosine_eps = 1e-06
LOG2E = 1.4426950408889634
F32 = jnp.float32
BF16 = jnp.bfloat16
INTERPRET = False


def dot(a, b, ca, cb):
    return lax.dot_general(a, b, (((ca,), (cb,)), ((), ())), preferred_element_type=F32)


def split2(x):
    hi = x.astype(BF16)
    lo = (x - hi.astype(F32)).astype(BF16)
    return hi, lo


def split3(x):
    hi = x.astype(BF16)
    r = x - hi.astype(F32)
    mid = r.astype(BF16)
    lo = (r - mid.astype(F32)).astype(BF16)
    return hi, mid, lo


def dot22(a, b, ca, cb):
    ah, al = split2(a)
    bh, bl = split2(b)
    return dot(ah, bh, ca, cb) + dot(ah, bl, ca, cb) + dot(al, bh, ca, cb)


def dot33(a, b, ca, cb):
    ah, am, al = split3(a)
    bh, bm, bl = split3(b)
    small = dot(ah, bl, ca, cb) + dot(al, bh, ca, cb) + dot(am, bm, ca, cb)
    return small + (dot(ah, bm, ca, cb) + dot(am, bh, ca, cb)) + dot(ah, bh, ca, cb)


def iota(shape, axis):
    return lax.broadcasted_iota(jnp.int32, shape, axis)


def call(body, out_shape, in_specs=None, out_specs=None, scratch=(), **kw):
    return pl.pallas_call(
        body,
        out_shape=out_shape,
        in_specs=in_specs,
        out_specs=out_specs,
        scratch_shapes=scratch,
        interpret=INTERPRET,
        compiler_params=pltpu.CompilerParams(vmem_limit_bytes=56 << 20),
        **kw,
    )


def vmem():
    return pl.BlockSpec(memory_space=pltpu.VMEM)


def smem():
    return pl.BlockSpec(memory_space=pltpu.SMEM)


def conv_body(f_ref, w_ref, o_ref):
    y = dot(w_ref[...], f_ref[...], 1, 1)
    tiles = []
    for ky in range(3):
        for h in range(8):
            tiles.append(
                jnp.concatenate(
                    [
                        y[(ky * 3 + kx) * 8 : (ky * 3 + kx) * 8 + 8, h * 128 : h * 128 + 128]
                        for kx in range(3)
                    ],
                    axis=1,
                )
            )
    a = jnp.concatenate(tiles, axis=0)
    row = iota((384, 128), 0)
    col = iota((384, 128), 1)
    w = 2 * (col % 64) + col // 64
    pick = jnp.where(row % 128 == w + row // 128 - 1, 1.0, 0.0).astype(BF16)
    hi, mid, lo = split3(a)
    z = dot(lo, pick, 1, 0) + dot(mid, pick, 1, 0) + dot(hi, pick, 1, 0)

    def latent(r):
        acc = None
        for ky in range(3):
            h = r + ky - 1
            if 0 <= h < 8:
                part = z[(ky * 8 + h) * 8 : (ky * 8 + h) * 8 + 8]
                acc = part if acc is None else acc + part
        return acc

    for i in range(-1, 5):
        parts = []
        if 2 * i >= -1 and 2 * i <= 8:
            parts.append(latent(2 * i))
        if 2 * i + 1 >= -1 and 2 * i + 1 <= 8:
            parts.append(pltpu.roll(latent(2 * i + 1), 4, 0))
        o_ref[(i + 1) * 8 : (i + 2) * 8, :] = sum(parts[1:], parts[0])


def weights_body(lab_ref, e_ref, mod_ref, qkv_ref, outw_ref, m_ref, b_ref, c_ref, ep_ref):
    lab = lab_ref[0]
    rows = mod_ref[...].astype(F32)
    pickrow = iota(rows.shape, 0) == lab % 8
    mod = jnp.sum(jnp.where(pickrow, rows, 0.0), axis=0, keepdims=True)
    shift = mod[:, :1024]
    scale = mod[:, 1024:]
    r = iota((16, 16), 0)
    c = iota((16, 16), 1)
    src = (r // 4 % 2) * 8 + (r // 8) * 4 + r % 4
    perm = jnp.where(c == src, 1.0, 0.0).astype(BF16)
    ef = dot(perm, e_ref[...], 1, 0)
    ep_ref[...] = ef.astype(BF16)
    ec = ef - jnp.mean(ef, axis=1, keepdims=True)
    m_ref[...] = dot33(ec, ec, 1, 1) * (1.0 / 1024)
    hi, mid, lo = split3(ec * (1.0 + scale))
    sh = jnp.where(iota((16, 1024), 0) == 0, shift, 0.0).astype(BF16)
    full = dot(jnp.concatenate([hi, mid, lo, sh], axis=0), qkv_ref[...], 1, 0)
    a = full[:16] + full[16:32] + full[32:48]
    bias = full[48:49]
    aq, ak, av = a[:, :1024], a[:, 1024:2048], a[:, 2048:]
    bq, bk, bv = bias[:, :1024], bias[:, 1024:2048], bias[:, 2048:]
    r16 = iota((16, 1024), 0)
    qexp = jnp.concatenate([aq, jnp.where(r16 == 0, bq, 0.0)], axis=0)
    kexp = jnp.concatenate([ak, ak, ak, jnp.where(r16 < 3, bk, 0.0)], axis=0)
    vexp = jnp.concatenate([av, av, jnp.zeros_like(av), jnp.where(r16 < 3, bv, 0.0)], axis=0)
    even = iota((64, 128), 1) < 64
    for p in range(8):
        s = slice(128 * p, 128 * p + 128)
        k2 = kexp[:, s]
        k4 = jnp.concatenate([jnp.where(even, k2, 0.0), jnp.where(even, 0.0, k2)], axis=0)
        b_ref[:, s] = dot33(qexp[:, s], k4, 1, 1) * (LOG2E / 8.0)
        v2 = vexp[:, s]
        v4 = jnp.concatenate([jnp.where(even, v2, 0.0), jnp.where(even, 0.0, v2)], axis=0)
        hi, lo = split2(v4)
        w = outw_ref[s, :]
        c_ref[s, :] = (dot(hi, w, 1, 0) + dot(lo, w, 1, 0)).astype(BF16)


def lane64(shape):
    return iota(shape, 1) % 64


def with_bias(x, base):
    hi, mid, lo = split3(x)
    col = lane64(x.shape)
    out = jnp.where(col < 48, base.astype(F32), 0.0)
    out = jnp.where(col == 48, hi.astype(F32), out)
    out = jnp.where(col == 49, mid.astype(F32), out)
    out = jnp.where(col == 50, lo.astype(F32), out)
    return out.astype(BF16)


def forward_body(
    s_ref, t0_ref, t1_ref, t2_ref, t3_ref, m_ref, b_ref, c_ref, ep_ref, pw_ref, d_ref,
    gp_ref, gz_ref, w_out, x_out, uk_out, ut_out, vt_out, inv_out, loss_ref,
    tbuf, tok, own, wsel,
):
    s = s_ref[0]
    for k, ref in enumerate((t0_ref, t1_ref, t2_ref, t3_ref)):
        tbuf[(s + 4 - k) % 4] = ref[...]
    left = iota((8, 128), 1) < 64

    def patch_row(t):
        a, i = t // 4, t % 4
        v = tbuf[a, 8 * (i + 1) : 8 * (i + 2), :]
        if i == 3 and a < 3:
            v = v + tbuf[a + 1, 0:8, :]
        if i == 0 and a > 0:
            v = v + tbuf[a - 1, 40:48, :]
        return v * latent_scale

    for j in range(8):
        ta, tb = patch_row(2 * j), patch_row(2 * j + 1)
        tok[0:8, 128 * j : 128 * j + 128] = jnp.where(left, ta, pltpu.roll(tb, 64, 1))
        tok[8:16, 128 * j : 128 * j + 128] = jnp.where(left, pltpu.roll(ta, 64, 1), tb)
    tokt = tok[...]
    v = dot33(m_ref[...], tokt, 1, 0)
    inv = lax.rsqrt(jnp.sum(tokt * v, axis=0, keepdims=True) + norm_eps)
    ut = tokt * inv
    vt = v * inv
    ut_out[...] = ut
    vt_out[...] = vt
    inv_out[...] = jnp.broadcast_to(inv, (8, 1024))
    uh, ul = split2(ut)
    ones = jnp.where(iota((16, 1024), 0) < 3, 1.0, 0.0).astype(BF16)
    uk_out[...] = jnp.concatenate([uh, ul, uh, ones], axis=0)
    for a in range(4):
        own[a, 0:16, :] = tokt[:, 256 * a : 256 * a + 256]
        own[a, 16:32, :] = ut[:, 256 * a : 256 * a + 256]
    mine = own[s]
    tok_own, u_own = mine[0:16], mine[16:32]
    uoh, uol = split2(u_own)
    one16 = jnp.where(iota((16, 256), 0) == 0, 1.0, 0.0).astype(BF16)
    zero16 = jnp.zeros((16, 256), BF16)
    lhs = jnp.concatenate([uoh, one16, uoh, one16, uol, zero16], axis=0)
    bh, bl = split2(b_ref[...])
    wall = dot(lhs, jnp.concatenate([bh, bl, bh], axis=0), 0, 0)
    hi = wall.astype(BF16)
    rest = (wall - hi.astype(F32)).astype(BF16)
    base = jnp.where(lane64(wall.shape) < 32, hi.astype(F32), rest.astype(F32))
    sel = with_bias(wall, base)
    for p in range(8):
        wsel[p] = sel[:, 128 * p : 128 * p + 128]
        w_out[p] = wall[:, 128 * p : 128 * p + 128]
    zk = jnp.zeros((64, 1024), BF16)
    uk = uk_out[...]
    uke = jnp.concatenate([uk, zk], axis=0)
    uko = jnp.concatenate([zk, uk], axis=0)
    lane = iota((256, 128), 1)

    def pair(p, carry):
        w = wsel[p]
        x = None
        tops = []
        for u in (uke, uko):
            sc = dot(w, u, 1, 0)
            top = jnp.max(sc, axis=1, keepdims=True)
            e = jnp.exp2(sc - top).astype(BF16)
            part = dot(e, u, 1, 1)
            x = part if x is None else x + part
            tops.append(top)
        t0, t1 = x[:, 48:49], x[:, 112:113]
        total = jnp.where(lane < 64, t0, t1)
        top = jnp.where(lane < 64, tops[0], tops[1])
        lse = top + jnp.log2(total)
        x_out[p] = jnp.where(lane % 64 < 49, x / total, 0.0).astype(BF16)
        w_out[p] = jnp.where(lane % 64 >= 48, w_out[p] - lse, w_out[p])
        return carry

    lax.fori_loop(0, 8, pair, 0)
    xn = jnp.concatenate([x_out[p] for p in range(8)], axis=1)
    th, tm, tl = split3(tok_own)
    ep = ep_ref[...]
    start = dot(jnp.concatenate([th, tm, tl], axis=0), jnp.concatenate([ep, ep, ep], axis=0), 0, 0)
    resid = start + dot(xn, c_ref[...], 1, 0)
    rb = resid.astype(BF16)
    zp = dot(rb, pw_ref[...], 1, 0)
    d = d_ref[...].astype(F32)
    nz2 = jnp.sum(zp * zp, axis=1, keepdims=True) + cosine_eps
    nd2 = jnp.sum(d * d, axis=1, keepdims=True) + cosine_eps
    zd = jnp.sum(zp * d, axis=1, keepdims=True)
    both = lax.rsqrt(nz2) * lax.rsqrt(nd2)
    cosine = zd * both
    gz = ((cosine / nz2) * zp - both * d).astype(BF16)
    gz_ref[...] = gz
    loss_ref[...] = jnp.broadcast_to(jnp.sum(1.0 - cosine, axis=0, keepdims=True), (8, 128))
    gp_ref[...] = dot(rb, gz, 0, 0).astype(gp_ref.dtype)


def backward_body(
    s_ref, gz_ref, w_ref, x_ref, uk_ref, ut_ref, vt_ref, inv_ref, b_ref, c_ref, ep_ref, pw_ref,
    o_ref,
    wsel, gsel, wt, gt, ysc, hk, hv, padded,
):
    s = s_ref[0]
    gresid = dot(gz_ref[...], pw_ref[...], 1, 1)
    gh, gl = split2(gresid)
    ep = ep_ref[...]
    r_own = dot(ep, gh, 1, 1) + dot(ep, gl, 1, 1)
    gexp = dot(gh, c_ref[...], 1, 1)
    r128 = iota((128, 128), 0) // 64
    c128 = iota((128, 128), 1) // 64
    block = jnp.where(r128 == c128, 1.0, 0.0).astype(BF16)
    col = iota((256, 128), 1) % 64
    for p in range(8):
        g = gexp[:, 128 * p : 128 * p + 128]
        g_hi = g.astype(BF16).astype(F32)
        ph, plo = split2(g_hi * x_ref[p].astype(F32))
        delta = dot(ph, block, 1, 0) + dot(plo, block, 1, 0)
        gs = with_bias(g_hi - delta, jnp.where(col < 32, g_hi, 0.0))
        gsel[p] = gs
        gt[p] = gs.astype(F32).T.astype(BF16)
        w = w_ref[p]
        hi = w.astype(BF16).astype(F32)
        ws = with_bias(w, jnp.where(col < 32, hi, w - hi))
        wsel[p] = ws
        wt[p] = ws.astype(F32).T.astype(BF16)
    hk[...] = jnp.zeros_like(hk)
    hv[...] = jnp.zeros_like(hv)
    uk = uk_ref[...]
    zk = jnp.zeros((64, 1024), BF16)
    uke = jnp.concatenate([uk, zk], axis=0)
    uko = jnp.concatenate([zk, uk], axis=0)

    def pair(p, carry):
        w = wsel[p]
        g = gsel[p]
        y = None
        for half, u in enumerate((uke, uko)):
            prob = jnp.exp2(dot(w, u, 1, 0))
            ds = (prob * dot(g, u, 1, 0)).astype(BF16)
            pb = prob.astype(BF16)
            part = dot(ds, u, 1, 1)
            y = part if y is None else y + part
            hk[...] += dot(wt[p, 64 * half : 64 * half + 16, :], ds, 1, 0)
            hv[...] += dot(gt[p, 64 * half : 64 * half + 16, :], pb, 1, 0)
        ysc[p] = jnp.where((col < 32) | (col == 48), y, 0.0)
        return carry

    lax.fori_loop(0, 8, pair, 0)
    y = jnp.concatenate([ysc[p] for p in range(8)], axis=1)
    ln2 = 1.0 / LOG2E
    hq = dot22(b_ref[...], y, 1, 1)[0:16] * ln2
    h = hk[...] * ln2 + hv[...]
    own = padded
    for a in range(4):
        mineq = jnp.where(s == a, 1.0, 0.0)
        own[a, :, 0:256] = h[:, 256 * a : 256 * a + 256] + mineq * hq
    h = jnp.concatenate([own[a, :, 0:256] for a in range(4)], axis=1)
    ut = ut_ref[...]
    inv = inv_ref[0:1, :]
    g = inv * (h - vt_ref[...] * jnp.sum(ut * h, axis=0, keepdims=True))
    z = jnp.zeros((16, 128), F32)
    pieces = []
    for a in range(4):
        mineq = jnp.where(s == a, 1.0, 0.0)
        pieces.append((g[:, 256 * a : 256 * a + 256] + mineq * r_own) * latent_scale)
    line = jnp.concatenate([z] + pieces + [z], axis=1)
    for a in range(4):
        padded[a] = line[:, 256 * a : 256 * a + 512]
    for k in range(4):
        o_ref[k] = padded[(s + k) % 4]


def output_body(g0_ref, g1_ref, g2_ref, g3_ref, f_ref, w_ref, o_ref, gc_ref):
    g = (g0_ref[...] + g1_ref[...] + g2_ref[...] + g3_ref[...]).astype(BF16).astype(F32)
    left = iota((8, 128), 1) < 64
    tiles = []
    for j in range(4):
        x0 = g[0:8, 128 * j : 128 * j + 128]
        x1 = g[8:16, 128 * j : 128 * j + 128]
        tiles.append(jnp.where(left, x0, pltpu.roll(x1, 64, 1)))
        tiles.append(jnp.where(left, pltpu.roll(x0, 64, 1), x1))
    t = jnp.concatenate(tiles[1:7], axis=0).astype(BF16)
    q = iota((128, 384), 0)
    col = iota((128, 384), 1)
    pick = jnp.where(2 * (q % 64) + q // 64 == col % 128 + 1 - col // 128, 1.0, 0.0).astype(BF16)
    v = dot(t, pick, 1, 0)

    def tile(i, kx):
        return v[8 * (i + 1) : 8 * (i + 2), 128 * kx : 128 * kx + 128]

    acc = [None, None]
    for a in range(8):
        i = a // 2
        other = i - 1 if a % 2 == 0 else i + 1
        rows = []
        for kx in range(3):
            rows += [tile(i, kx), tile(other, kx)]
        gt = jnp.concatenate(rows, axis=0).astype(BF16)
        o_ref[128 * a : 128 * a + 128, :] = dot(gt, w_ref[a % 2], 0, 0).astype(BF16)
        part = dot(gt, f_ref[128 * a : 128 * a + 128, :], 1, 0)
        acc[a % 2] = part if acc[a % 2] is None else acc[a % 2] + part
    ev, od = acc
    for kx in range(3):
        et, epv = ev[16 * kx : 16 * kx + 8], ev[16 * kx + 8 : 16 * kx + 16]
        ot, on = od[16 * kx : 16 * kx + 8], od[16 * kx + 8 : 16 * kx + 16]
        gc_ref[kx] = pltpu.roll(et, 4, 0) + on
        gc_ref[3 + kx] = et + pltpu.roll(ot, 4, 0)
        gc_ref[6 + kx] = pltpu.roll(epv, 4, 0) + ot


def shifted(x, axis, n, k):
    return lax.ppermute(x, axis, [(i, (i + k) % n) for i in range(n)])


SLAB = ("xh", "core")
CHIPS = ("xh", "z", "y", "xl")


def reduced(parts):
    n = parts.shape[-1]
    core = lax.axis_index("core")
    halves = parts.reshape(2, 64, 8, n)
    mine = lax.dynamic_index_in_dim(halves, core, 0, keepdims=False)
    other = lax.dynamic_index_in_dim(halves, 1 - core, 0, keepdims=False)
    got = shifted(other, "core", 2, 1)
    chip = (mine.astype(F32) + got.astype(F32)).astype(BF16)
    pieces = lax.all_to_all(chip, CHIPS, split_axis=0, concat_axis=0, tiled=True)
    return jnp.sum(pieces.astype(F32), 0)


def gathered(block):
    n = block.shape[-1]
    same = jnp.broadcast_to(block[None], (64, 8, n))
    half = lax.all_to_all(same, CHIPS, split_axis=0, concat_axis=0, tiled=True)
    other = shifted(half, "core", 2, 1)
    core = lax.axis_index("core")
    return jnp.where(core == 0, half, other), jnp.where(core == 0, other, half)


def local(feats, labels, conv_w, embed_w, mod_table, qkv_w, out_w, proj_w, dino):
    slab = (lax.axis_index("xh") * 2 + lax.axis_index("core")).astype(jnp.int32).reshape(1)
    image = feats.reshape(1024, 512)
    taps = conv_w.transpose(0, 2, 1)
    w72 = jnp.pad(taps, ((0, 0), (0, 4), (0, 0))).reshape(72, 512)
    t3 = taps.reshape(3, 3, 4, 512)
    none = jnp.zeros_like(t3[0])
    w_even = jnp.stack([t3[1], t3[0], none, t3[2]], axis=1).reshape(48, 512)
    w_odd = jnp.stack([t3[2], t3[1], t3[0], none], axis=1).reshape(48, 512)
    w_back = jnp.stack([w_even, w_odd])

    part = call(
        conv_body, jax.ShapeDtypeStruct((48, 128), F32), [vmem(), vmem()], vmem()
    )(image, w72)
    parts = [part] + [shifted(part, SLAB, 4, k) for k in (1, 2, 3)]

    mat, bexp, cexp, ep = pl.pallas_call(
        weights_body,
        out_shape=(
            jax.ShapeDtypeStruct((16, 16), F32),
            jax.ShapeDtypeStruct((32, 1024), F32),
            jax.ShapeDtypeStruct((1024, 1024), BF16),
            jax.ShapeDtypeStruct((16, 1024), BF16),
        ),
        grid_spec=pltpu.PrefetchScalarGridSpec(
            num_scalar_prefetch=1,
            grid=(1,),
            in_specs=[
                pl.BlockSpec((16, 1024), lambda i, lab: (0, 0)),
                pl.BlockSpec((8, 2048), lambda i, lab: (lab[0] // 8, 0)),
                pl.BlockSpec((1024, 3072), lambda i, lab: (0, 0)),
                pl.BlockSpec((1024, 1024), lambda i, lab: (0, 0)),
            ],
            out_specs=[
                pl.BlockSpec((16, 16), lambda i, lab: (0, 0)),
                pl.BlockSpec((32, 1024), lambda i, lab: (0, 0)),
                pl.BlockSpec((1024, 1024), lambda i, lab: (0, 0)),
                pl.BlockSpec((16, 1024), lambda i, lab: (0, 0)),
            ],
        ),
        interpret=INTERPRET,
        compiler_params=pltpu.CompilerParams(vmem_limit_bytes=56 << 20),
    )(labels, embed_w, mod_table, qkv_w, out_w)

    gp, gz, w_all, x_all, uk, ut, vt, inv, loss = call(
        forward_body,
        (
            jax.ShapeDtypeStruct((1024, 768), BF16),
            jax.ShapeDtypeStruct((256, 768), BF16),
            jax.ShapeDtypeStruct((8, 256, 128), F32),
            jax.ShapeDtypeStruct((8, 256, 128), BF16),
            jax.ShapeDtypeStruct((64, 1024), BF16),
            jax.ShapeDtypeStruct((16, 1024), F32),
            jax.ShapeDtypeStruct((16, 1024), F32),
            jax.ShapeDtypeStruct((8, 1024), F32),
            jax.ShapeDtypeStruct((8, 128), F32),
        ),
        [smem()] + [vmem()] * 10,
        tuple([vmem()] * 9),
        scratch=[
            pltpu.VMEM((4, 48, 128), F32),
            pltpu.VMEM((16, 1024), F32),
            pltpu.VMEM((4, 32, 256), F32),
            pltpu.VMEM((8, 256, 128), BF16),
        ],
    )(slab, *parts, mat, bexp, cexp, ep, proj_w, dino.reshape(256, 768))

    pieces = call(
        backward_body,
        jax.ShapeDtypeStruct((4, 16, 512), F32),
        [smem()] + [vmem()] * 11,
        vmem(),
        scratch=[
            pltpu.VMEM((8, 256, 128), BF16),
            pltpu.VMEM((8, 256, 128), BF16),
            pltpu.VMEM((8, 128, 256), BF16),
            pltpu.VMEM((8, 128, 256), BF16),
            pltpu.VMEM((8, 256, 128), F32),
            pltpu.VMEM((16, 1024), F32),
            pltpu.VMEM((16, 1024), F32),
            pltpu.VMEM((4, 16, 512), F32),
        ],
    )(slab, gz, w_all, x_all, uk, ut, vt, inv, bexp, cexp, ep, proj_w)
    grads = [pieces[0]] + [shifted(pieces[k], SLAB, 4, k) for k in (1, 2, 3)]

    grad_image, gconv = call(
        output_body,
        (jax.ShapeDtypeStruct((1024, 512), BF16), jax.ShapeDtypeStruct((9, 8, 512), F32)),
        [vmem()] * 6,
        (vmem(), vmem()),
    )(*grads, image, w_back)

    conv_part = gconv.astype(BF16).reshape(9, 8, 4, 128).transpose(0, 2, 1, 3).reshape(36, 8, 128)
    total = loss[0, 0]
    lh, lm, ll = split3(total)
    lane = jnp.arange(128)
    loss_row = jnp.where(lane == 0, lh, jnp.where(lane == 1, lm, jnp.where(lane == 2, ll, 0)))
    loss_part = jnp.broadcast_to(loss_row.astype(BF16), (1, 8, 128))
    extra = jnp.concatenate([conv_part, loss_part, jnp.zeros((91, 8, 128), BF16)])
    both = jnp.concatenate([gp.reshape(128, 8, 768), extra], axis=2)
    block = reduced(both)
    lsum = jnp.sum(block[0, 768:771])
    lh, lm, ll = split3(lsum)
    pos = (lax.axis_index(CHIPS) + 64 * lax.axis_index("core")) == 36
    wide = jnp.arange(896)[None, :]
    coded = jnp.where(wide == 768, lh, jnp.where(wide == 769, lm, ll)).astype(BF16)
    is_loss = pos & (wide >= 768) & (wide < 771)
    block = jnp.where(is_loss, coded, block.astype(BF16))
    first, second = gathered(block)
    grad_proj = jnp.concatenate([first[:, :, :768], second[:, :, :768]]).reshape(1024, 768).astype(F32)
    conv = first[:36, :4, 768:].astype(F32).reshape(9, 4, 4, 128).transpose(0, 2, 1, 3)
    grad_conv = conv.reshape(9, 4, 512).transpose(0, 2, 1)
    loss_sum = jnp.sum(first[36, 0, 768:771].astype(F32))
    return (
        grad_image.reshape(1, 8, 128, 512),
        grad_proj,
        grad_conv,
        loss_sum / 32768.0,
    )


def solution(mesh):
    fine = Mesh(mesh.devices.reshape(2, 2, 4, 4, 2), ("xh", "core", "z", "y", "xl"))
    img = ("z", "y", "xl")
    in_specs = (
        P(img, SLAB, None, None), P(img), P(), P(), P(), P(), P(), P(), P(img, SLAB, None),
    )
    out_specs = (P(img, SLAB, None, None), P(), P(), P())
    return jax.shard_map(local, mesh=fine, in_specs=in_specs, out_specs=out_specs, check_vma=False)
```

```python
import functools
import jax
import jax.numpy as jnp
from jax import lax
from jax.experimental import pallas as pl
from jax.experimental.pallas import tpu as pltpu
from jax.sharding import Mesh
from jax.sharding import PartitionSpec as P

HEAD_DIM = 64
latent_scale = 0.18215
norm_eps = 1e-06
cosine_eps = 1e-06
LOG2E = 1.4426950408889634
F32 = jnp.float32
BF16 = jnp.bfloat16
INTERPRET = False


def dot(a, b, ca, cb):
    return lax.dot_general(a, b, (((ca,), (cb,)), ((), ())), preferred_element_type=F32)


def split2(x):
    hi = x.astype(BF16)
    lo = (x - hi.astype(F32)).astype(BF16)
    return hi, lo


def split3(x):
    hi = x.astype(BF16)
    r = x - hi.astype(F32)
    mid = r.astype(BF16)
    lo = (r - mid.astype(F32)).astype(BF16)
    return hi, mid, lo


def dot22(a, b, ca, cb):
    ah, al = split2(a)
    bh, bl = split2(b)
    return dot(ah, bh, ca, cb) + dot(ah, bl, ca, cb) + dot(al, bh, ca, cb)


def dot33(a, b, ca, cb):
    ah, am, al = split3(a)
    bh, bm, bl = split3(b)
    small = dot(ah, bl, ca, cb) + dot(al, bh, ca, cb) + dot(am, bm, ca, cb)
    return small + (dot(ah, bm, ca, cb) + dot(am, bh, ca, cb)) + dot(ah, bh, ca, cb)


def iota(shape, axis):
    return lax.broadcasted_iota(jnp.int32, shape, axis)


def call(body, out_shape, in_specs=None, out_specs=None, scratch=(), **kw):
    return pl.pallas_call(
        body,
        out_shape=out_shape,
        in_specs=in_specs,
        out_specs=out_specs,
        scratch_shapes=scratch,
        interpret=INTERPRET,
        compiler_params=pltpu.CompilerParams(vmem_limit_bytes=56 << 20),
        **kw,
    )


def vmem():
    return pl.BlockSpec(memory_space=pltpu.VMEM)


def smem():
    return pl.BlockSpec(memory_space=pltpu.SMEM)


def spread(w_ref, rows, source):
    acc = None
    for t in range(9):
        r = iota((rows, 4), 0)
        pick = jnp.where(source(r) == 4 * t + iota((rows, 4), 1), 1.0, 0.0).astype(BF16)
        part = dot(pick, w_ref[t], 1, 0)
        acc = part if acc is None else acc + part
    return acc.astype(BF16)


def conv_body(f_ref, w_ref, o_ref):
    w72 = spread(w_ref, 72, lambda r: jnp.where(r % 8 < 4, r // 8 * 4 + r % 8, -1))
    y = dot(w72, f_ref[...], 1, 1)
    tiles = []
    for ky in range(3):
        for h in range(8):
            tiles.append(
                jnp.concatenate(
                    [
                        y[(ky * 3 + kx) * 8 : (ky * 3 + kx) * 8 + 8, h * 128 : h * 128 + 128]
                        for kx in range(3)
                    ],
                    axis=1,
                )
            )
    a = jnp.concatenate(tiles, axis=0)
    row = iota((384, 128), 0)
    col = iota((384, 128), 1)
    w = 2 * (col % 64) + col // 64
    pick = jnp.where(row % 128 == w + row // 128 - 1, 1.0, 0.0).astype(BF16)
    hi, mid, lo = split3(a)
    z = dot(lo, pick, 1, 0) + dot(mid, pick, 1, 0) + dot(hi, pick, 1, 0)

    def latent(r):
        acc = None
        for ky in range(3):
            h = r + ky - 1
            if 0 <= h < 8:
                part = z[(ky * 8 + h) * 8 : (ky * 8 + h) * 8 + 8]
                acc = part if acc is None else acc + part
        return acc

    for i in range(-1, 5):
        parts = []
        if 2 * i >= -1 and 2 * i <= 8:
            parts.append(latent(2 * i))
        if 2 * i + 1 >= -1 and 2 * i + 1 <= 8:
            parts.append(pltpu.roll(latent(2 * i + 1), 4, 0))
        o_ref[(i + 1) * 8 : (i + 2) * 8, :] = sum(parts[1:], parts[0])


def weights_body(lab_ref, e_ref, mod_ref, qkv_ref, outw_ref, m_ref, b_ref, c_ref, ep_ref):
    lab = lab_ref[0]
    rows = mod_ref[...].astype(F32)
    pickrow = iota(rows.shape, 0) == lab % 8
    mod = jnp.sum(jnp.where(pickrow, rows, 0.0), axis=0, keepdims=True)
    shift = mod[:, :1024]
    scale = mod[:, 1024:]
    r = iota((16, 16), 0)
    c = iota((16, 16), 1)
    src = (r // 4 % 2) * 8 + (r // 8) * 4 + r % 4
    perm = jnp.where(c == src, 1.0, 0.0).astype(BF16)
    ef = dot(perm, e_ref[...], 1, 0)
    ep_ref[...] = ef.astype(BF16)
    ec = ef - jnp.mean(ef, axis=1, keepdims=True)
    m_ref[...] = dot33(ec, ec, 1, 1) * (1.0 / 1024)
    hi, mid, lo = split3(ec * (1.0 + scale))
    sh = jnp.where(iota((16, 1024), 0) == 0, shift, 0.0).astype(BF16)
    full = dot(jnp.concatenate([hi, mid, lo, sh], axis=0), qkv_ref[...], 1, 0)
    a = full[:16] + full[16:32] + full[32:48]
    bias = full[48:49]
    aq, ak, av = a[:, :1024], a[:, 1024:2048], a[:, 2048:]
    bq, bk, bv = bias[:, :1024], bias[:, 1024:2048], bias[:, 2048:]
    r16 = iota((16, 1024), 0)
    qexp = jnp.concatenate([aq, jnp.where(r16 == 0, bq, 0.0)], axis=0)
    kexp = jnp.concatenate([ak, ak, ak, jnp.where(r16 < 3, bk, 0.0)], axis=0)
    vexp = jnp.concatenate([av, av, jnp.zeros_like(av), jnp.where(r16 < 3, bv, 0.0)], axis=0)
    even = iota((64, 128), 1) < 64
    for p in range(8):
        s = slice(128 * p, 128 * p + 128)
        k2 = kexp[:, s]
        k4 = jnp.concatenate([jnp.where(even, k2, 0.0), jnp.where(even, 0.0, k2)], axis=0)
        b_ref[:, s] = dot33(qexp[:, s], k4, 1, 1) * (LOG2E / 8.0)
        v2 = vexp[:, s]
        v4 = jnp.concatenate([jnp.where(even, v2, 0.0), jnp.where(even, 0.0, v2)], axis=0)
        hi, lo = split2(v4)
        w = outw_ref[s, :]
        c_ref[s, :] = (dot(hi, w, 1, 0) + dot(lo, w, 1, 0)).astype(BF16)


def lane64(shape):
    return iota(shape, 1) % 64


def with_bias(x, base):
    hi, mid, lo = split3(x)
    col = lane64(x.shape)
    out = jnp.where(col < 48, base.astype(F32), 0.0)
    out = jnp.where(col == 48, hi.astype(F32), out)
    out = jnp.where(col == 49, mid.astype(F32), out)
    out = jnp.where(col == 50, lo.astype(F32), out)
    return out.astype(BF16)


def forward_body(
    s_ref, t0_ref, t1_ref, t2_ref, t3_ref, m_ref, b_ref, c_ref, ep_ref, pw_ref, d_ref,
    gp_ref, gz_ref, w_out, x_out, uk_out, ut_out, vt_out, inv_out, loss_ref,
    tbuf, tok, own, wsel,
):
    s = s_ref[0]
    for k, ref in enumerate((t0_ref, t1_ref, t2_ref, t3_ref)):
        tbuf[(s + 4 - k) % 4] = ref[...]
    left = iota((8, 128), 1) < 64

    def patch_row(t):
        a, i = t // 4, t % 4
        v = tbuf[a, 8 * (i + 1) : 8 * (i + 2), :]
        if i == 3 and a < 3:
            v = v + tbuf[a + 1, 0:8, :]
        if i == 0 and a > 0:
            v = v + tbuf[a - 1, 40:48, :]
        return v * latent_scale

    for j in range(8):
        ta, tb = patch_row(2 * j), patch_row(2 * j + 1)
        tok[0:8, 128 * j : 128 * j + 128] = jnp.where(left, ta, pltpu.roll(tb, 64, 1))
        tok[8:16, 128 * j : 128 * j + 128] = jnp.where(left, pltpu.roll(ta, 64, 1), tb)
    tokt = tok[...]
    v = dot33(m_ref[...], tokt, 1, 0)
    inv = lax.rsqrt(jnp.sum(tokt * v, axis=0, keepdims=True) + norm_eps)
    ut = tokt * inv
    vt = v * inv
    ut_out[...] = ut
    vt_out[...] = vt
    inv_out[...] = jnp.broadcast_to(inv, (8, 1024))
    uh, ul = split2(ut)
    ones = jnp.where(iota((16, 1024), 0) < 3, 1.0, 0.0).astype(BF16)
    uk_out[...] = jnp.concatenate([uh, ul, uh, ones], axis=0)
    for a in range(4):
        own[a, 0:16, :] = tokt[:, 256 * a : 256 * a + 256]
        own[a, 16:32, :] = ut[:, 256 * a : 256 * a + 256]
    mine = own[s]
    tok_own, u_own = mine[0:16], mine[16:32]
    uoh, uol = split2(u_own)
    one16 = jnp.where(iota((16, 256), 0) == 0, 1.0, 0.0).astype(BF16)
    zero16 = jnp.zeros((16, 256), BF16)
    lhs = jnp.concatenate([uoh, one16, uoh, one16, uol, zero16], axis=0)
    bh, bl = split2(b_ref[...])
    wall = dot(lhs, jnp.concatenate([bh, bl, bh], axis=0), 0, 0)
    hi = wall.astype(BF16)
    rest = (wall - hi.astype(F32)).astype(BF16)
    base = jnp.where(lane64(wall.shape) < 32, hi.astype(F32), rest.astype(F32))
    sel = with_bias(wall, base)
    for p in range(8):
        wsel[p] = sel[:, 128 * p : 128 * p + 128]
        w_out[p] = wall[:, 128 * p : 128 * p + 128]
    zk = jnp.zeros((64, 1024), BF16)
    uk = uk_out[...]
    uke = jnp.concatenate([uk, zk], axis=0)
    uko = jnp.concatenate([zk, uk], axis=0)
    lane = iota((256, 128), 1)

    def pair(p, carry):
        w = wsel[p]
        x = None
        tops = []
        for u in (uke, uko):
            sc = dot(w, u, 1, 0)
            top = jnp.max(sc, axis=1, keepdims=True)
            e = jnp.exp2(sc - top).astype(BF16)
            part = dot(e, u, 1, 1)
            x = part if x is None else x + part
            tops.append(top)
        t0, t1 = x[:, 48:49], x[:, 112:113]
        total = jnp.where(lane < 64, t0, t1)
        top = jnp.where(lane < 64, tops[0], tops[1])
        lse = top + jnp.log2(total)
        x_out[p] = jnp.where(lane % 64 < 49, x / total, 0.0).astype(BF16)
        w_out[p] = jnp.where(lane % 64 >= 48, w_out[p] - lse, w_out[p])
        return carry

    lax.fori_loop(0, 8, pair, 0)
    xn = jnp.concatenate([x_out[p] for p in range(8)], axis=1)
    th, tm, tl = split3(tok_own)
    ep = ep_ref[...]
    start = dot(jnp.concatenate([th, tm, tl], axis=0), jnp.concatenate([ep, ep, ep], axis=0), 0, 0)
    resid = start + dot(xn, c_ref[...], 1, 0)
    rb = resid.astype(BF16)
    zp = dot(rb, pw_ref[...], 1, 0)
    d = d_ref[...].astype(F32)
    nz2 = jnp.sum(zp * zp, axis=1, keepdims=True) + cosine_eps
    nd2 = jnp.sum(d * d, axis=1, keepdims=True) + cosine_eps
    zd = jnp.sum(zp * d, axis=1, keepdims=True)
    both = lax.rsqrt(nz2) * lax.rsqrt(nd2)
    cosine = zd * both
    gz = ((cosine / nz2) * zp - both * d).astype(BF16)
    gz_ref[...] = gz
    loss_ref[...] = jnp.broadcast_to(jnp.sum(1.0 - cosine, axis=0, keepdims=True), (8, 128))
    gp_ref[...] = dot(rb, gz, 0, 0).astype(gp_ref.dtype)


def backward_body(
    s_ref, gz_ref, w_ref, x_ref, uk_ref, ut_ref, vt_ref, inv_ref, b_ref, c_ref, ep_ref, pw_ref,
    o0_ref, o1_ref, o2_ref, o3_ref,
    wsel, gsel, wt, gt, ysc, hk, hv, padded,
):
    s = s_ref[0]
    gresid = dot(gz_ref[...], pw_ref[...], 1, 1)
    gh, gl = split2(gresid)
    ep = ep_ref[...]
    r_own = dot(ep, gh, 1, 1) + dot(ep, gl, 1, 1)
    gexp = dot(gh, c_ref[...], 1, 1)
    r128 = iota((128, 128), 0) // 64
    c128 = iota((128, 128), 1) // 64
    block = jnp.where(r128 == c128, 1.0, 0.0).astype(BF16)
    col = iota((256, 128), 1) % 64
    for p in range(8):
        g = gexp[:, 128 * p : 128 * p + 128]
        g_hi = g.astype(BF16).astype(F32)
        ph, plo = split2(g_hi * x_ref[p].astype(F32))
        delta = dot(ph, block, 1, 0) + dot(plo, block, 1, 0)
        gs = with_bias(g_hi - delta, jnp.where(col < 32, g_hi, 0.0))
        gsel[p] = gs
        gt[p] = gs.astype(F32).T.astype(BF16)
        w = w_ref[p]
        hi = w.astype(BF16).astype(F32)
        ws = with_bias(w, jnp.where(col < 32, hi, w - hi))
        wsel[p] = ws
        wt[p] = ws.astype(F32).T.astype(BF16)
    hk[...] = jnp.zeros_like(hk)
    hv[...] = jnp.zeros_like(hv)
    uk = uk_ref[...]
    zk = jnp.zeros((64, 1024), BF16)
    uke = jnp.concatenate([uk, zk], axis=0)
    uko = jnp.concatenate([zk, uk], axis=0)

    def pair(p, carry):
        w = wsel[p]
        g = gsel[p]
        y = None
        for half, u in enumerate((uke, uko)):
            prob = jnp.exp2(dot(w, u, 1, 0))
            ds = (prob * dot(g, u, 1, 0)).astype(BF16)
            pb = prob.astype(BF16)
            part = dot(ds, u, 1, 1)
            y = part if y is None else y + part
            hk[...] += dot(wt[p, 64 * half : 64 * half + 16, :], ds, 1, 0)
            hv[...] += dot(gt[p, 64 * half : 64 * half + 16, :], pb, 1, 0)
        ysc[p] = jnp.where((col < 32) | (col == 48), y, 0.0)
        return carry

    lax.fori_loop(0, 8, pair, 0)
    y = jnp.concatenate([ysc[p] for p in range(8)], axis=1)
    ln2 = 1.0 / LOG2E
    hq = dot22(b_ref[...], y, 1, 1)[0:16] * ln2
    h = hk[...] * ln2 + hv[...]
    own = padded
    for a in range(4):
        mineq = jnp.where(s == a, 1.0, 0.0)
        own[a, :, 0:256] = h[:, 256 * a : 256 * a + 256] + mineq * hq
    h = jnp.concatenate([own[a, :, 0:256] for a in range(4)], axis=1)
    ut = ut_ref[...]
    inv = inv_ref[0:1, :]
    g = inv * (h - vt_ref[...] * jnp.sum(ut * h, axis=0, keepdims=True))
    z = jnp.zeros((16, 128), F32)
    pieces = []
    for a in range(4):
        mineq = jnp.where(s == a, 1.0, 0.0)
        pieces.append((g[:, 256 * a : 256 * a + 256] + mineq * r_own) * latent_scale)
    line = jnp.concatenate([z] + pieces + [z], axis=1)
    for a in range(4):
        padded[a] = line[:, 256 * a : 256 * a + 512]
    for k, ref in enumerate((o0_ref, o1_ref, o2_ref, o3_ref)):
        ref[...] = padded[(s + k) % 4]


def output_body(g0_ref, g1_ref, g2_ref, g3_ref, f_ref, w_ref, loss_ref, o_ref, gc_ref):
    def even_tap(r):
        kx, q, o = r // 16, r % 16 // 4, r % 4
        ky = jnp.where(q == 0, 1, jnp.where(q == 1, 0, 2))
        return jnp.where(q == 2, -1, (ky * 3 + kx) * 4 + o)

    def odd_tap(r):
        kx, q, o = r // 16, r % 16 // 4, r % 4
        return jnp.where(q == 3, -1, ((2 - q) * 3 + kx) * 4 + o)

    w_back = (spread(w_ref, 48, even_tap), spread(w_ref, 48, odd_tap))
    g = (g0_ref[...] + g1_ref[...] + g2_ref[...] + g3_ref[...]).astype(BF16).astype(F32)
    left = iota((8, 128), 1) < 64
    tiles = []
    for j in range(4):
        x0 = g[0:8, 128 * j : 128 * j + 128]
        x1 = g[8:16, 128 * j : 128 * j + 128]
        tiles.append(jnp.where(left, x0, pltpu.roll(x1, 64, 1)))
        tiles.append(jnp.where(left, pltpu.roll(x0, 64, 1), x1))
    t = jnp.concatenate(tiles[1:7], axis=0).astype(BF16)
    q = iota((128, 384), 0)
    col = iota((128, 384), 1)
    pick = jnp.where(2 * (q % 64) + q // 64 == col % 128 + 1 - col // 128, 1.0, 0.0).astype(BF16)
    v = dot(t, pick, 1, 0)

    def tile(i, kx):
        return v[8 * (i + 1) : 8 * (i + 2), 128 * kx : 128 * kx + 128]

    acc = [None, None]
    for a in range(8):
        i = a // 2
        other = i - 1 if a % 2 == 0 else i + 1
        rows = []
        for kx in range(3):
            rows += [tile(i, kx), tile(other, kx)]
        gt = jnp.concatenate(rows, axis=0).astype(BF16)
        o_ref[128 * a : 128 * a + 128, :] = dot(gt, w_back[a % 2], 0, 0).astype(BF16)
        part = dot(gt, f_ref[128 * a : 128 * a + 128, :], 1, 0)
        acc[a % 2] = part if acc[a % 2] is None else acc[a % 2] + part
    ev, od = acc
    taps = [None] * 9
    for kx in range(3):
        et, epv = ev[16 * kx : 16 * kx + 8], ev[16 * kx + 8 : 16 * kx + 16]
        ot, on = od[16 * kx : 16 * kx + 8], od[16 * kx + 8 : 16 * kx + 16]
        taps[kx] = pltpu.roll(et, 4, 0) + on
        taps[3 + kx] = et + pltpu.roll(ot, 4, 0)
        taps[6 + kx] = pltpu.roll(epv, 4, 0) + ot
    upper = iota((8, 512), 0) < 4
    rows = [
        jnp.where(upper, taps[2 * j], pltpu.roll(taps[2 * j + 1], 4, 0)) for j in range(4)
    ]
    rows.append(jnp.where(upper, taps[8], 0.0))
    put_sum(gc_ref, jnp.concatenate(rows, axis=0), loss_ref[0:1, 0:1])


def put_sum(ref, conv, total):
    hi, mid, lo = split3(total)
    row = iota((40, 512), 0)
    lane = iota((40, 512), 1)
    loss = jnp.where(lane == 0, hi.astype(F32), 0.0)
    loss = jnp.where(lane == 1, mid.astype(F32), loss)
    loss = jnp.where(lane == 2, lo.astype(F32), loss)
    ref[...] = jnp.where(row == 36, loss, jnp.where(row < 36, conv, 0.0)).astype(BF16)


def sum_refs(refs):
    acc = refs[0][...].astype(F32)
    for ref in refs[1:]:
        acc = acc + ref[...].astype(F32)
    return acc, jnp.sum(acc[36:37, 0:128], axis=1, keepdims=True)


def merge_body(*refs):
    conv, total = sum_refs(refs[:-1])
    put_sum(refs[-1], conv, total)


def finish_body(*refs):
    conv, total = sum_refs(refs[:-2])
    for t in range(9):
        refs[-2][t] = conv[4 * t : 4 * t + 4]
    refs[-1][...] = jnp.broadcast_to(total * (1.0 / 32768.0), (8, 128))


def shifted(x, axis, n, k):
    return lax.ppermute(x, axis, [(i, (i + k) % n) for i in range(n)])


SLAB = ("xh", "core")
ALL = ("xh", "core", "z", "y", "xl")


def summed(conv, axis, n, last):
    parts = [conv] + [shifted(conv, axis, n, k) for k in range(1, n)]
    if not last:
        return call(merge_body, jax.ShapeDtypeStruct((40, 512), BF16), [vmem()] * n, vmem())(*parts)
    return call(
        finish_body,
        (jax.ShapeDtypeStruct((9, 4, 512), F32), jax.ShapeDtypeStruct((8, 128), F32)),
        [vmem()] * n,
        (vmem(), vmem()),
    )(*parts)


def local(feats, labels, conv_w, embed_w, mod_table, qkv_w, out_w, proj_w, dino):
    slab = (lax.axis_index("xh") * 2 + lax.axis_index("core")).astype(jnp.int32).reshape(1)
    image = feats.reshape(1024, 512)
    taps = conv_w.transpose(0, 2, 1)
    part = call(
        conv_body, jax.ShapeDtypeStruct((48, 128), F32), [vmem(), vmem()], vmem()
    )(image, taps)
    parts = [part] + [shifted(part, SLAB, 4, k) for k in (1, 2, 3)]

    mat, bexp, cexp, ep = pl.pallas_call(
        weights_body,
        out_shape=(
            jax.ShapeDtypeStruct((16, 16), F32),
            jax.ShapeDtypeStruct((32, 1024), F32),
            jax.ShapeDtypeStruct((1024, 1024), BF16),
            jax.ShapeDtypeStruct((16, 1024), BF16),
        ),
        grid_spec=pltpu.PrefetchScalarGridSpec(
            num_scalar_prefetch=1,
            grid=(1,),
            in_specs=[
                pl.BlockSpec((16, 1024), lambda i, lab: (0, 0)),
                pl.BlockSpec((8, 2048), lambda i, lab: (lab[0] // 8, 0)),
                pl.BlockSpec((1024, 3072), lambda i, lab: (0, 0)),
                pl.BlockSpec((1024, 1024), lambda i, lab: (0, 0)),
            ],
            out_specs=[
                pl.BlockSpec((16, 16), lambda i, lab: (0, 0)),
                pl.BlockSpec((32, 1024), lambda i, lab: (0, 0)),
                pl.BlockSpec((1024, 1024), lambda i, lab: (0, 0)),
                pl.BlockSpec((16, 1024), lambda i, lab: (0, 0)),
            ],
        ),
        interpret=INTERPRET,
        compiler_params=pltpu.CompilerParams(vmem_limit_bytes=56 << 20),
    )(labels, embed_w, mod_table, qkv_w, out_w)

    gp, gz, w_all, x_all, uk, ut, vt, inv, loss = call(
        forward_body,
        (
            jax.ShapeDtypeStruct((1024, 768), BF16),
            jax.ShapeDtypeStruct((256, 768), BF16),
            jax.ShapeDtypeStruct((8, 256, 128), F32),
            jax.ShapeDtypeStruct((8, 256, 128), BF16),
            jax.ShapeDtypeStruct((64, 1024), BF16),
            jax.ShapeDtypeStruct((16, 1024), F32),
            jax.ShapeDtypeStruct((16, 1024), F32),
            jax.ShapeDtypeStruct((8, 1024), F32),
            jax.ShapeDtypeStruct((8, 128), F32),
        ),
        [smem()] + [vmem()] * 10,
        tuple([vmem()] * 9),
        scratch=[
            pltpu.VMEM((4, 48, 128), F32),
            pltpu.VMEM((16, 1024), F32),
            pltpu.VMEM((4, 32, 256), F32),
            pltpu.VMEM((8, 256, 128), BF16),
        ],
    )(slab, *parts, mat, bexp, cexp, ep, proj_w, dino.reshape(256, 768))

    parts = lax.all_to_all(gp.reshape(128, 8, 768), ALL, split_axis=0, concat_axis=0, tiled=True)
    block = jnp.sum(parts.astype(F32), 0).astype(BF16)
    same = jnp.broadcast_to(block[None], (128, 8, 768))
    whole = lax.all_to_all(same, ALL, split_axis=0, concat_axis=0, tiled=True)
    grad_proj = whole.reshape(1024, 768).astype(F32)

    pieces = call(
        backward_body,
        tuple([jax.ShapeDtypeStruct((16, 512), F32)] * 4),
        [smem()] + [vmem()] * 11,
        tuple([vmem()] * 4),
        scratch=[
            pltpu.VMEM((8, 256, 128), BF16),
            pltpu.VMEM((8, 256, 128), BF16),
            pltpu.VMEM((8, 128, 256), BF16),
            pltpu.VMEM((8, 128, 256), BF16),
            pltpu.VMEM((8, 256, 128), F32),
            pltpu.VMEM((16, 1024), F32),
            pltpu.VMEM((16, 1024), F32),
            pltpu.VMEM((4, 16, 512), F32),
        ],
    )(slab, gz, w_all, x_all, uk, ut, vt, inv, bexp, cexp, ep, proj_w)
    grads = [pieces[0]] + [shifted(pieces[k], SLAB, 4, k) for k in (1, 2, 3)]

    grad_image, conv = call(
        output_body,
        (jax.ShapeDtypeStruct((1024, 512), BF16), jax.ShapeDtypeStruct((40, 512), BF16)),
        [vmem()] * 7,
        (vmem(), vmem()),
    )(*grads, image, taps, loss)
    conv = summed(conv, "z", 4, False)
    conv = summed(conv, "y", 4, False)
    conv, loss = summed(conv, ("xh", "core", "xl"), 8, True)
    return (
        grad_image.reshape(1, 8, 128, 512),
        grad_proj,
        conv.transpose(0, 2, 1),
        loss[0, 0],
    )


def solution(mesh):
    fine = Mesh(mesh.devices.reshape(2, 2, 4, 4, 2), ("xh", "core", "z", "y", "xl"))
    img = ("z", "y", "xl")
    in_specs = (
        P(img, SLAB, None, None), P(img), P(), P(), P(), P(), P(), P(), P(img, SLAB, None),
    )
    out_specs = (P(img, SLAB, None, None), P(), P(), P())
    return jax.shard_map(local, mesh=fine, in_specs=in_specs, out_specs=out_specs, check_vma=False)
```
